256 devices in a mesh: space: 32 (over z_hi, x, core), chan: 8 (over y, z_lo).
Axes of the slice: x: 4, y: 4, z: 8 (z_hi: 4, z_lo: 2; z = z_hi * 2 + z_lo), core: 2. Of those that a mesh axis runs over, the one named last changes fastest.
Arguments:
- patches: bfloat16 [64, 8192, 1024], P('chan', 'space'), may hold values from -6 to 6
- var_embed: float32 [64, 1024], P('chan'), may hold values from -3 to 3
- agg_query: float32 [1024], replicated, may hold values from -18 to 18
- pos_embed: bfloat16 [8192, 1024], P('space'), may hold values from -3 to 3
- gain_first: float32 [1024], replicated, may hold values from 0.1 to 1.9
- gain_second: float32 [1024], replicated, may hold values from 0.1 to 1.9
- w_qkv: bfloat16 [1024, 3, 1024], P(None, None, 'chan'), may hold values from -0.3 to 0.3
- w_out: bfloat16 [1024, 1024], P('chan'), may hold values from -0.1875 to 0.1875
- w_dec: bfloat16 [1024, 1024], replicated, may hold values from -0.1875 to 0.1875
- mod_scale: float32 [64, 1024], P('chan'), may hold values from -3 to 3
- mod_shift: float32 [64, 1024], P('chan'), may hold values from -3 to 3
Outputs:
- decoded: bfloat16 [64, 8192, 1024], P('chan', 'space')
The draws below stay inside these ranges and needn't reach their ends.
All inputs are finite; a program needn't handle non-finite values.
Results may differ from the reference program's by a relative error of at most 0.025.
Values may be sent and summed in bfloat16 or wider, within the bound.
No kernel may reach another device: no remote copies, remote signals or barrier semaphores. Data moves between devices by JAX's collectives and lax.ppermute only.
A program may use at most 64 MiB of HBM per device.

```python
import math
import jax
import jax.numpy as jnp
from jax import lax

D = 1024
HEADS = 16
VARS = 64
POSITIONS = 8192


weight_bound = 0.296875


def query_vector(key):
    base = jax.random.normal(jax.random.fold_in(key, 11), (D,), jnp.float32)
    return jnp.clip(3.0 * base, -18.0, 18.0)


def variable_rows(key):
    base = jax.random.normal(jax.random.fold_in(key, 12), (VARS, D), jnp.float32)
    return jnp.clip(0.5 * base, -3.0, 3.0)


def draw_agg_query(key, part):
    return query_vector(key)


def draw_var_embed(key, part):
    return variable_rows(key)


def draw_patches(key, part):
    noise = jnp.clip(jax.random.normal(jax.random.fold_in(key, 13), (VARS, POSITIONS, D), jnp.float32), -6.0, 6.0)
    return noise.astype(jnp.bfloat16)


def draw_w_qkv(key, part):
    scale = 1.5 / math.sqrt(D)
    base = jnp.clip(jax.random.normal(jax.random.fold_in(key, 15), (D, 3, D), jnp.float32), -6.0, 6.0) * scale
    base = jnp.clip(base, -weight_bound, weight_bound)
    return base.astype(jnp.bfloat16)


def steps_of(stream_key, extent, pieces, least, largest):
    def one(position, blocks):
        steps = jax.random.uniform(jax.random.fold_in(jax.random.fold_in(stream_key, 6), position), (blocks,), jnp.float32, least / len(pieces), largest / len(pieces))
        return jnp.repeat(jnp.exp(steps), extent[position] // blocks).reshape((-1,) + (1,) * (len(extent) - position - 1))

    loudness = one(*pieces[0])
    for cut in pieces[1:]:
        loudness = loudness * one(*cut)
    return loudness


def centred(rng, shape, scale, limit, shards=(), dtype=jnp.bfloat16):
    drawn = jax.random.normal(rng, shape, jnp.float32) * scale
    if len(shards) > 0:
        drawn = steps_of(rng, shape, shards, -0.22, 0.18) * drawn
    return jnp.clip(drawn, min=-limit, max=limit).astype(dtype)


def setup_inputs(seed: int = 0) -> dict:
    arg_keys = jax.random.split(jax.random.key(seed), 12)
    patches = draw_patches(jax.random.fold_in(arg_keys[11], 71), 0)
    var_embed = draw_var_embed(jax.random.fold_in(arg_keys[11], 71), 0)
    agg_query = draw_agg_query(jax.random.fold_in(arg_keys[11], 71), 0)
    pos_embed = centred(arg_keys[3], (POSITIONS, D), 0.5, 3.0, ((0, 32),))
    gain_first = jnp.clip(1.0 + 0.18 * jax.random.normal(arg_keys[4], (D,), jnp.float32), 0.1, 1.9)
    gain_second = jnp.clip(1.0 + 0.18 * jax.random.normal(arg_keys[5], (D,), jnp.float32), 0.1, 1.9)
    w_qkv = draw_w_qkv(jax.random.fold_in(arg_keys[11], 71), 0)
    w_out = centred(arg_keys[7], (D, D), D ** -0.5, 0.1875, ((0, 8),))
    w_dec = centred(arg_keys[8], (D, D), D ** -0.5, 0.1875)
    mod_scale = centred(arg_keys[9], (VARS, D), 0.5, 3.0, ((0, 8),), jnp.float32)
    mod_shift = centred(arg_keys[10], (VARS, D), 0.5, 3.0, ((0, 8),), jnp.float32)
    return dict(patches=patches, var_embed=var_embed, agg_query=agg_query, pos_embed=pos_embed, gain_first=gain_first, gain_second=gain_second, w_qkv=w_qkv, w_out=w_out, w_dec=w_dec, mod_scale=mod_scale, mod_shift=mod_shift)


epsilon = 1e-06

def rms_norm(values, gain_vec):
    return values * lax.rsqrt(lax.optimization_barrier(jnp.mean(values * values, -1, keepdims=True)) + epsilon) * gain_vec

def reference(patches, var_embed, agg_query, pos_embed, gain_first, gain_second, w_qkv, w_out, w_dec, mod_scale, mod_shift):
    agg_scale = 1.0 / math.sqrt(D)

    def var_logit(pair_in):
        tokens_var, embed_var = pair_in
        embedded = tokens_var.astype(jnp.float32) + embed_var
        return lax.optimization_barrier(jnp.sum(embedded * agg_query, -1)) * agg_scale
    logits = lax.map(var_logit, (patches, var_embed))
    agg_weights = jax.nn.softmax(logits, axis=0)

    def add_var(running, triple_in):
        tokens_var, embed_var, weight_var = triple_in
        embedded = tokens_var.astype(jnp.float32) + embed_var
        return (running + weight_var[:, None] * embedded, None)
    pooled, _ = lax.scan(add_var, jnp.zeros((POSITIONS, D), jnp.float32), (patches, var_embed, agg_weights))
    resid = pooled + pos_embed.astype(jnp.float32)
    normed = rms_norm(resid, gain_first).astype(jnp.bfloat16)
    qkv_all = jnp.dot(normed, w_qkv.reshape(D, 3 * D), preferred_element_type=jnp.float32).astype(jnp.bfloat16)
    head_dim = D // HEADS
    queries = qkv_all[:, :D].reshape(POSITIONS, HEADS, head_dim).transpose(1, 0, 2)
    keys_all = qkv_all[:, D:2 * D].reshape(POSITIONS, HEADS, head_dim).transpose(1, 0, 2)
    values_all = qkv_all[:, 2 * D:].reshape(POSITIONS, HEADS, head_dim).transpose(1, 0, 2)
    inv_scale = 1.0 / math.sqrt(head_dim)

    def one_head(triple_in):
        query_head, key_head, value_head = triple_in
        scores = jnp.dot(query_head, key_head.T, preferred_element_type=jnp.float32) * inv_scale
        probs = jax.nn.softmax(scores, axis=-1).astype(jnp.bfloat16)
        return jnp.dot(probs, value_head, preferred_element_type=jnp.float32).astype(jnp.bfloat16)
    mixed = lax.map(one_head, (queries, keys_all, values_all)).transpose(1, 0, 2).reshape(POSITIONS, D)
    trunk = resid + jnp.dot(mixed, w_out, preferred_element_type=jnp.float32)
    normed_two = rms_norm(trunk, gain_second).astype(jnp.bfloat16)

    def decode_var(pair_in):
        scale_var, shift_var = pair_in
        modulated = (normed_two.astype(jnp.float32) * (1.0 + scale_var) + shift_var).astype(jnp.bfloat16)
        return jnp.dot(modulated, w_dec, preferred_element_type=jnp.float32).astype(jnp.bfloat16)
    return lax.map(decode_var, (mod_scale, mod_shift))
```

```python
import functools
import math

import jax
import jax.numpy as jnp
from jax import lax
from jax.experimental import pallas as pl
from jax.experimental.pallas import tpu as pltpu
from jax.sharding import PartitionSpec as P

D = 1024
HEADS = 16
HEAD_DIM = D // HEADS
EPS = 1e-6
LOG2E = 1.4426950408889634
Z_HI, X, CORES = 4, 4, 2
F32, BF16 = jnp.float32, jnp.bfloat16

VMEM = pl.BlockSpec(memory_space=pltpu.VMEM)
SMEM = pl.BlockSpec(memory_space=pltpu.SMEM)


def shape(dims, dtype):
    return jax.ShapeDtypeStruct(dims, dtype)


def in_three(value):
    high = value.astype(BF16)
    rest = value - high.astype(F32)
    mid = rest.astype(BF16)
    low = (rest - mid.astype(F32)).astype(BF16)
    return high.astype(F32), mid.astype(F32), low.astype(F32)


def pool_kernel(patches, var_embed, query, out):
    count = patches.shape[0]
    rows = patches.shape[1]
    scaled = query[...] * (LOG2E / math.sqrt(D))
    logits = []
    for v in range(count):
        embedded = patches[v].astype(F32) + var_embed[v : v + 1, :]
        logits.append(jnp.sum(embedded * scaled, -1, keepdims=True))
    top = functools.reduce(jnp.maximum, logits)
    expo = [jnp.exp2(l - top) for l in logits]
    total = functools.reduce(jnp.add, expo)
    acc = jnp.zeros((rows, D), F32)
    for v in range(count):
        embedded = patches[v].astype(F32) + var_embed[v : v + 1, :]
        acc = acc + (expo[v] / total) * embedded
    out[0, :, :D] = acc.astype(BF16)
    high, mid, low = in_three(top + jnp.log2(total))
    lane = lax.broadcasted_iota(jnp.int32, (rows, 128), 1)
    packed = jnp.where(lane == 0, high, jnp.where(lane == 1, mid, jnp.where(lane == 2, low, 0.0)))
    out[0, :, D:] = packed.astype(BF16)


def pool(patches, var_embed, query, peers):
    count, rows, _ = patches.shape
    part = rows // peers
    return pl.pallas_call(
        pool_kernel,
        grid=(peers,),
        in_specs=[
            pl.BlockSpec((count, part, D), lambda i: (0, i, 0)),
            pl.BlockSpec((count, D), lambda i: (0, 0)),
            pl.BlockSpec((1, D), lambda i: (0, 0)),
        ],
        out_specs=pl.BlockSpec((1, part, D + 128), lambda i: (i, 0, 0)),
        out_shape=shape((peers, part, D + 128), BF16),
        name="pool",
    )(patches, var_embed, query)


def merge_pool_kernel(me, parts, pos, gain, resid, normed):
    peers, rows, _ = parts.shape
    logs = [jnp.sum(parts[i, :, D:].astype(F32), -1, keepdims=True) for i in range(peers)]
    top = functools.reduce(jnp.maximum, logs)
    weights = [jnp.exp2(l - top) for l in logs]
    total = functools.reduce(jnp.add, weights)
    acc = jnp.zeros((rows, D), F32)
    for i in range(peers):
        acc = acc + (weights[i] / total) * parts[i, :, :D].astype(F32)
    start = pl.multiple_of(me[0] * rows, rows)
    value = acc + pos[pl.ds(start, rows), :].astype(F32)
    resid[...] = value
    mean = jnp.mean(value * value, -1, keepdims=True)
    result = (value * lax.rsqrt(mean + EPS) * gain[...]).astype(BF16)
    for i in range(peers):
        normed[i] = result


def merge_pool(me, parts, pos, gain):
    peers, rows, _ = parts.shape
    return pl.pallas_call(
        merge_pool_kernel,
        in_specs=[SMEM, VMEM, VMEM, VMEM],
        out_specs=(VMEM, VMEM),
        out_shape=(shape((rows, D), F32), shape((peers, rows, D), BF16)),
        name="merge_pool",
    )(me, parts, pos, gain)


def project_kernel(core, normed, weight, mine, other):
    rows = normed.shape[0]
    x = normed[...]
    q, k, v = (jnp.dot(x, weight[i], preferred_element_type=F32) for i in range(3))
    low = lax.broadcasted_iota(jnp.int32, (rows, 2 * HEAD_DIM), 1) < HEAD_DIM
    first = jnp.where(low, k, pltpu.roll(v, HEAD_DIM, 1))
    second = jnp.where(low, pltpu.roll(k, HEAD_DIM, 1), v)
    is_first = core[0] == 0
    turned = (q * (1.0 / math.sqrt(HEAD_DIM))).T
    top, bottom = turned[:HEAD_DIM], turned[HEAD_DIM:]
    half = rows // 2
    for ref, kv, qt in (
        (mine, jnp.where(is_first, first, second), jnp.where(is_first, top, bottom)),
        (other, jnp.where(is_first, second, first), jnp.where(is_first, bottom, top)),
    ):
        ref[:rows, :] = kv.astype(BF16)
        ref[rows : rows + HEAD_DIM, :] = qt[:, :half].astype(BF16)
        ref[rows + HEAD_DIM :, :] = qt[:, half:].astype(BF16)


def project(core, normed, weight):
    rows = normed.shape[0]
    out = shape((rows + 2 * HEAD_DIM, 128), BF16)
    return pl.pallas_call(
        project_kernel,
        in_specs=[SMEM, VMEM, VMEM],
        out_specs=(VMEM, VMEM),
        out_shape=(out, out),
        name="project",
    )(core, normed, weight)


def attend_kernel(k0, k1, k2, k3, q0, q1, q2, q3, o0, o1, o2, o3, keys, values_t):
    each = k0.shape[0]
    for i, ref in enumerate((k0, k1, k2, k3)):
        block = ref[...]
        keys[i * each : (i + 1) * each, :] = block
        values_t[:, i * each : (i + 1) * each] = block.T[HEAD_DIM:, :]
    scale = LOG2E
    zeros = jnp.zeros((HEAD_DIM, 256), BF16)
    for q, o in zip((q0, q1, q2, q3), (o0, o1, o2, o3)):
        for half in range(2):
            at = half * 2 * HEAD_DIM
            qt = jnp.concatenate([q[at : at + HEAD_DIM, :], q[at + HEAD_DIM : at + 2 * HEAD_DIM, :]], 1)
            qt = jnp.concatenate([qt, zeros], 0)
            scores = jnp.dot(keys[...], qt, preferred_element_type=F32)
            top = jnp.max(scores, 0, keepdims=True)
            probs = jnp.exp2((scores - top) * scale)
            total = jnp.sum(probs, 0, keepdims=True)
            acc = jnp.dot(values_t[...], probs.astype(BF16), preferred_element_type=F32)
            lanes = slice(half * 256, half * 256 + 256)
            o[:HEAD_DIM, lanes] = (acc / total).astype(BF16)
            high, mid, low = in_three(top * scale + jnp.log2(total))
            row = lax.broadcasted_iota(jnp.int32, (16, 256), 0)
            packed = jnp.where(row == 0, high, jnp.where(row == 1, mid, jnp.where(row == 2, low, 0.0)))
            o[HEAD_DIM:, lanes] = packed.astype(BF16)


def attend(key_pieces, query_pieces):
    each = key_pieces[0].shape[0]
    out = shape((HEAD_DIM + 16, each), BF16)
    return pl.pallas_call(
        attend_kernel,
        in_specs=[VMEM] * 8,
        out_specs=(VMEM,) * 4,
        out_shape=(out,) * 4,
        scratch_shapes=[
            pltpu.VMEM((4 * each, 128), BF16),
            pltpu.VMEM((HEAD_DIM, 4 * each), BF16),
        ],
        name="attend",
    )(*key_pieces, *query_pieces)


def merge_heads_kernel(p0, p1, p2, p3, mine, other):
    refs = (p0, p1, p2, p3)
    logs = [jnp.sum(r[HEAD_DIM:, :].astype(F32), 0, keepdims=True) for r in refs]
    top = functools.reduce(jnp.maximum, logs)
    weights = [jnp.exp2(l - top) for l in logs]
    total = functools.reduce(jnp.add, weights)
    acc = jnp.zeros((HEAD_DIM, p0.shape[1]), F32)
    for r, w in zip(refs, weights):
        acc = acc + (w / total) * r[:HEAD_DIM, :].astype(F32)
    half = p0.shape[1] // 2
    mine[...] = acc[:, :half].astype(BF16)
    other[...] = acc[:, half:].astype(BF16)


def merge_heads(parts):
    width = parts[0].shape[1] // 2
    out = shape((HEAD_DIM, width), BF16)
    return pl.pallas_call(
        merge_heads_kernel,
        in_specs=[VMEM] * 4,
        out_specs=(VMEM, VMEM),
        out_shape=(out, out),
        name="merge_heads",
    )(*parts)


def out_kernel(core, mine, other, weight, out):
    at = pl.multiple_of(core[0] * HEAD_DIM, HEAD_DIM)
    away = pl.multiple_of((1 - core[0]) * HEAD_DIM, HEAD_DIM)
    dims = (((0,), (0,)), ((), ()))
    total = lax.dot_general(mine[...], weight[pl.ds(at, HEAD_DIM), :], dims, preferred_element_type=F32)
    total += lax.dot_general(other[...], weight[pl.ds(away, HEAD_DIM), :], dims, preferred_element_type=F32)
    out[...] = total.astype(BF16)


def project_out(core, mine, other, weight):
    return pl.pallas_call(
        out_kernel,
        in_specs=[SMEM, VMEM, VMEM, VMEM],
        out_specs=VMEM,
        out_shape=shape((mine.shape[1], D), BF16),
        name="project_out",
    )(core, mine, other, weight)


def trunk_kernel(parts, resid, gain, normed):
    peers = parts.shape[0]
    value = resid[...]
    for i in range(peers):
        value = value + parts[i].astype(F32)
    mean = jnp.mean(value * value, -1, keepdims=True)
    result = (value * lax.rsqrt(mean + EPS) * gain[...]).astype(BF16)
    for i in range(peers):
        normed[i] = result


def trunk(parts, resid, gain):
    return pl.pallas_call(
        trunk_kernel,
        in_specs=[VMEM, VMEM, VMEM],
        out_specs=VMEM,
        out_shape=shape(parts.shape, BF16),
        name="trunk",
    )(parts, resid, gain)


def decode_kernel(normed, scale, shift, weight, out):
    v = pl.program_id(0)
    row = (1.0 + scale[pl.ds(v, 1), :], shift[pl.ds(v, 1), :])
    modulated = (normed[...].astype(F32) * row[0] + row[1]).astype(BF16)
    out[0] = jnp.dot(modulated, weight[...], preferred_element_type=F32).astype(BF16)


def decode(normed, scale, shift, weight):
    count, rows = scale.shape[0], normed.shape[0]
    return pl.pallas_call(
        decode_kernel,
        grid=(count,),
        in_specs=[VMEM, VMEM, VMEM, VMEM],
        out_specs=pl.BlockSpec((1, rows, D), lambda v: (v, 0, 0)),
        out_shape=shape((count, rows, D), BF16),
        name="decode",
    )(normed, scale, shift, weight)


def space_index(z, x, core):
    return (z * X + x) * CORES + core


def moves(step):
    return [
        (space_index(z, x, c), space_index(*step(z, x, c)))
        for z in range(Z_HI)
        for x in range(X)
        for c in range(CORES)
    ]


SWAP = moves(lambda z, x, c: (z, x, 1 - c))


def along_x(k):
    return moves(lambda z, x, c: (z, (x + k) % X, c))


def along_z(k):
    return moves(lambda z, x, c: ((z + k) % Z_HI, x, c))


def exchange(array):
    return lax.all_to_all(array, "chan", 0, 0, tiled=True)


def body(
    patches,
    var_embed,
    agg_query,
    pos_embed,
    gain_first,
    gain_second,
    w_qkv,
    w_out,
    w_dec,
    mod_scale,
    mod_shift,
):
    rows = patches.shape[1]
    peers = lax.axis_size("chan")
    me = lax.axis_index("chan").astype(jnp.int32).reshape(1)
    core = (lax.axis_index("space") % CORES).astype(jnp.int32).reshape(1)

    parts = exchange(pool(patches, var_embed, agg_query.reshape(1, D), peers))
    resid, normed = merge_pool(me, parts, pos_embed, gain_first.reshape(1, D))
    normed = exchange(normed).reshape(rows, D)

    mine, other = project(core, normed, w_qkv.transpose(1, 0, 2))
    swapped = lax.ppermute(other, "space", SWAP)
    kv = jnp.concatenate([mine[:rows], swapped[:rows]], 0)
    qt = jnp.concatenate([mine[rows:], swapped[rows:]], 0)
    query_pieces = [qt] + [lax.ppermute(qt, "space", along_z(k)) for k in range(1, Z_HI)]
    key_pieces = [kv] + [lax.ppermute(kv, "space", along_x(k)) for k in range(1, X)]
    partial = attend(key_pieces, query_pieces)
    back = [partial[0]] + [lax.ppermute(partial[k], "space", along_z(-k)) for k in range(1, Z_HI)]
    mine, other = merge_heads(back)
    swapped = lax.ppermute(other, "space", SWAP)
    terms = exchange(project_out(core, mine, swapped, w_out).reshape(peers, rows // peers, D))
    normed_two = exchange(trunk(terms, resid, gain_second.reshape(1, D))).reshape(rows, D)
    return decode(normed_two, mod_scale, mod_shift, w_dec)


def solution(mesh):
    placed = (
        P("chan", "space", None),
        P("chan", None),
        P(),
        P("space", None),
        P(),
        P(),
        P(None, None, "chan"),
        P("chan", None),
        P(),
        P("chan", None),
        P("chan", None),
    )
    return jax.shard_map(
        body, mesh=mesh, in_specs=placed, out_specs=P("chan", "space", None), check_vma=False
    )
```

```python
import functools
import math

import jax
import jax.numpy as jnp
from jax import lax
from jax.experimental import pallas as pl
from jax.experimental.pallas import tpu as pltpu
from jax.sharding import PartitionSpec as P


D = 1024
HEADS = 16
HEAD_DIM = D // HEADS
EPS = 1e-6
LOG2E = 1.4426950408889634
Z_HI, X, CORES = 4, 4, 2
F32, BF16 = jnp.float32, jnp.bfloat16

VMEM = pl.BlockSpec(memory_space=pltpu.VMEM)
ANY = pl.BlockSpec(memory_space=pl.ANY)
HBM = pl.BlockSpec(memory_space=pltpu.HBM)
PARAMS = pltpu.CompilerParams(vmem_limit_bytes=24 << 20)


def cost(flops, moved):
    return pl.CostEstimate(flops=flops, bytes_accessed=moved, transcendentals=0)


def shape(dims, dtype):
    return jax.ShapeDtypeStruct(dims, dtype)


def in_three(value):
    high = value.astype(BF16)
    rest = value - high.astype(F32)
    mid = rest.astype(BF16)
    low = (rest - mid.astype(F32)).astype(BF16)
    return high.astype(F32), mid.astype(F32), low.astype(F32)


def pool_kernel(patches, var_embed, query, out):
    count = patches.shape[0]
    rows = patches.shape[1]
    scaled = query[...] * (LOG2E / math.sqrt(D))
    shared = jnp.sum(var_embed[...] * scaled, -1, keepdims=True)
    logits = [
        jnp.sum(patches[v].astype(F32) * scaled, -1, keepdims=True) + shared[v : v + 1, :]
        for v in range(count)
    ]
    top = functools.reduce(jnp.maximum, logits)
    expo = [jnp.exp2(l - top) for l in logits]
    total = functools.reduce(jnp.add, expo)
    acc = jnp.zeros((rows, D), F32)
    for v in range(count):
        embedded = patches[v].astype(F32) + var_embed[v : v + 1, :]
        acc = acc + (expo[v] / total) * embedded
    out[0, :, :D] = acc.astype(BF16)
    high, mid, low = in_three(top + jnp.log2(total))
    lane = lax.broadcasted_iota(jnp.int32, (rows, 128), 1)
    packed = jnp.where(lane == 0, high, jnp.where(lane == 1, mid, jnp.where(lane == 2, low, 0.0)))
    out[0, :, D:] = packed.astype(BF16)


def pool(patches, var_embed, query, peers):
    count, rows, _ = patches.shape
    part = rows // peers
    return pl.pallas_call(
        pool_kernel,
        grid=(peers,),
        in_specs=[
            pl.BlockSpec((count, part, D), lambda i: (0, i, 0)),
            pl.BlockSpec((count, D), lambda i: (0, 0)),
            pl.BlockSpec((1, D), lambda i: (0, 0)),
        ],
        out_specs=pl.BlockSpec((1, part, D + 128), lambda i: (i, 0, 0)),
        out_shape=shape((peers, part, D + 128), BF16),
        cost_estimate=cost(16 << 20, 8 << 20),
        name="pool",
    )(patches, var_embed, query)


def merge_pool_kernel(parts, pos, resid):
    peers, rows, _ = parts.shape
    logs = [jnp.sum(parts[i, :, D:].astype(F32), -1, keepdims=True) for i in range(peers)]
    top = functools.reduce(jnp.maximum, logs)
    weights = [jnp.exp2(l - top) for l in logs]
    total = functools.reduce(jnp.add, weights)
    acc = jnp.zeros((rows, D), F32)
    for i in range(peers):
        acc = acc + (weights[i] / total) * parts[i, :, :D].astype(F32)
    start = pl.multiple_of(lax.axis_index("chan") * rows, rows)
    value = (acc + pos[pl.ds(start, rows), :].astype(F32)).astype(BF16)
    for i in range(peers):
        resid[i] = value


def merge_pool(parts, pos):
    peers, rows, _ = parts.shape
    return pl.pallas_call(
        merge_pool_kernel,
        in_specs=[VMEM, VMEM],
        out_specs=VMEM,
        out_shape=shape((peers, rows, D), BF16),
        compiler_params=PARAMS,
        cost_estimate=cost(4<< 20, 2<< 20),
        name="merge_pool",
    )(parts, pos)


def project_kernel(resid, gain, weight, w_out, mine, other, copies, sems):
    half = w_out.shape[0] // CORES
    start = pl.multiple_of(lax.axis_index("space") % CORES * half, half)
    share = w_out.at[pl.ds(start, half), :]
    moved = [pltpu.make_async_copy(share, copies.at[i], sems.at[i]) for i in range(copies.shape[0])]
    for copy in moved:
        copy.start()
    rows = resid.shape[0]
    value = resid[...].astype(F32)
    mean = jnp.mean(value * value, -1, keepdims=True)
    x = (value * lax.rsqrt(mean + EPS) * gain[...]).astype(BF16)
    q, k, v = (jnp.dot(x, weight[i], preferred_element_type=F32) for i in range(3))
    low = lax.broadcasted_iota(jnp.int32, (rows, 2 * HEAD_DIM), 1) < HEAD_DIM
    first = jnp.where(low, k, pltpu.roll(v, HEAD_DIM, 1))
    second = jnp.where(low, pltpu.roll(k, HEAD_DIM, 1), v)
    is_first = lax.axis_index("space") % CORES == 0
    turned = (q * (1.0 / math.sqrt(HEAD_DIM))).T
    top, bottom = turned[:HEAD_DIM], turned[HEAD_DIM:]
    half = rows // 2
    for ref, kv, qt in (
        (mine, jnp.where(is_first, first, second), jnp.where(is_first, top, bottom)),
        (other, jnp.where(is_first, second, first), jnp.where(is_first, bottom, top)),
    ):
        ref[:rows, :] = kv.astype(BF16)
        ref[rows : rows + HEAD_DIM, :] = qt[:, :half].astype(BF16)
        ref[rows + HEAD_DIM :, :] = qt[:, half:].astype(BF16)
    for copy in moved:
        copy.wait()


def project(resid, gain, weight, w_out, peers):
    rows = resid.shape[0]
    out = shape((rows + 2 * HEAD_DIM, 128), BF16)
    return pl.pallas_call(
        project_kernel,
        in_specs=[VMEM, VMEM, VMEM, VMEM],
        out_specs=(VMEM, VMEM, ANY),
        out_shape=(out, out, shape((peers, w_out.shape[0] // CORES, D), BF16)),
        scratch_shapes=[pltpu.SemaphoreType.DMA((peers,))],
        compiler_params=PARAMS,
        cost_estimate=cost(200 << 20, 4<< 20),
        name="project",
    )(resid, gain, weight, w_out)


def pair_kernel(mine, swapped, kv, qt):
    rows, turned = kv.shape[0] // 2, qt.shape[0] // 2
    kv[:rows, :] = mine[:rows, :]
    kv[rows:, :] = swapped[:rows, :]
    qt[:turned, :] = mine[rows:, :]
    qt[turned:, :] = swapped[rows:, :]


def pair(mine, swapped):
    rows = mine.shape[0] - 2 * HEAD_DIM
    return pl.pallas_call(
        pair_kernel,
        in_specs=[VMEM, VMEM],
        out_specs=(VMEM, VMEM),
        out_shape=(shape((2 * rows, 128), BF16), shape((4 * HEAD_DIM, 128), BF16)),
        compiler_params=PARAMS,
        cost_estimate=cost(1<< 20, 1<< 20),
        name="pair",
    )(mine, swapped)


def attend_kernel(k0, k1, k2, k3, q0, q1, q2, q3, o0, o1, o2, o3, keys, values_t):
    each = k0.shape[0]
    for i, ref in enumerate((k0, k1, k2, k3)):
        block = ref[...]
        keys[i * each : (i + 1) * each, :] = block
        values_t[:, i * each : (i + 1) * each] = block.T[HEAD_DIM:, :]
    scale = LOG2E
    zeros = jnp.zeros((HEAD_DIM, 256), BF16)
    for q, o in zip((q0, q1, q2, q3), (o0, o1, o2, o3)):
        for half in range(2):
            at = half * 2 * HEAD_DIM
            qt = jnp.concatenate([q[at : at + HEAD_DIM, :], q[at + HEAD_DIM : at + 2 * HEAD_DIM, :]], 1)
            qt = jnp.concatenate([qt, zeros], 0)
            scores = jnp.dot(keys[...], qt, preferred_element_type=F32)
            top = jnp.max(scores, 0, keepdims=True)
            probs = jnp.exp2((scores - top) * scale)
            total = jnp.sum(probs, 0, keepdims=True)
            acc = jnp.dot(values_t[...], probs.astype(BF16), preferred_element_type=F32)
            lanes = slice(half * 256, half * 256 + 256)
            o[:HEAD_DIM, lanes] = (acc / total).astype(BF16)
            high, mid, low = in_three(top * scale + jnp.log2(total))
            row = lax.broadcasted_iota(jnp.int32, (16, 256), 0)
            packed = jnp.where(row == 0, high, jnp.where(row == 1, mid, jnp.where(row == 2, low, 0.0)))
            o[HEAD_DIM:, lanes] = packed.astype(BF16)


def attend(key_pieces, query_pieces):
    each = key_pieces[0].shape[0]
    out = shape((HEAD_DIM + 16, each), BF16)
    return pl.pallas_call(
        attend_kernel,
        in_specs=[VMEM] * 8,
        out_specs=(VMEM,) * 4,
        out_shape=(out,) * 4,
        scratch_shapes=[
            pltpu.VMEM((4 * each, 128), BF16),
            pltpu.VMEM((HEAD_DIM, 4 * each), BF16),
        ],
        compiler_params=PARAMS,
        cost_estimate=cost(4 << 30, 8<< 20),
        name="attend",
    )(*key_pieces, *query_pieces)


def merge_heads_kernel(p0, p1, p2, p3, _, mine, other):
    refs = (p0, p1, p2, p3)
    logs = [jnp.sum(r[HEAD_DIM:, :].astype(F32), 0, keepdims=True) for r in refs]
    top = functools.reduce(jnp.maximum, logs)
    weights = [jnp.exp2(l - top) for l in logs]
    total = functools.reduce(jnp.add, weights)
    acc = jnp.zeros((HEAD_DIM, p0.shape[1]), F32)
    for r, w in zip(refs, weights):
        acc = acc + (w / total) * r[:HEAD_DIM, :].astype(F32)
    half = p0.shape[1] // 2
    mine[...] = acc[:, :half].astype(BF16)
    other[...] = acc[:, half:].astype(BF16)


def merge_heads(parts, after):
    width = parts[0].shape[1] // 2
    out = shape((HEAD_DIM, width), BF16)
    return pl.pallas_call(
        merge_heads_kernel,
        in_specs=[VMEM] * 4 + [ANY],
        out_specs=(VMEM, VMEM),
        out_shape=(out, out),
        compiler_params=PARAMS,
        cost_estimate=cost(1<< 20, 1<< 20),
        name="merge_heads",
    )(*parts, after)


def spread_kernel(mine, other, out):
    both = jnp.concatenate([mine[...].astype(F32), other[...].astype(F32)], 0)
    value = both.T.astype(BF16)
    for i in range(out.shape[0]):
        out[i] = value


def spread(mine, other, peers):
    return pl.pallas_call(
        spread_kernel,
        in_specs=[VMEM, VMEM],
        out_specs=VMEM,
        out_shape=shape((peers, mine.shape[1], 2 * HEAD_DIM), BF16),
        compiler_params=PARAMS,
        cost_estimate=cost(1<< 20, 1<< 20),
        name="spread",
    )(mine, other)


def decode_kernel(mixed, w_mine, w_other, resid, gain, scale, shift, w_dec, out, normed, weight, sem):
    step = pl.program_id(0)
    each = out.shape[0]

    @pl.when(step == 0)
    def _():
        copy = pltpu.make_async_copy(w_dec, weight, sem)
        copy.start()
        heads = jnp.concatenate([mixed[i] for i in range(mixed.shape[0])], 1)
        weights = [ref[i] for i in range(mixed.shape[0]) for ref in (w_mine, w_other)]
        value = jnp.dot(heads, jnp.concatenate(weights, 0), preferred_element_type=F32)
        value = value + resid[...].astype(F32)
        mean = jnp.mean(value * value, -1, keepdims=True)
        normed[...] = (value * lax.rsqrt(mean + EPS) * gain[...]).astype(BF16)
        copy.wait()

    parts = []
    for i in range(each):
        v = step * each + i
        row = (1.0 + scale[pl.ds(v, 1), :], shift[pl.ds(v, 1), :])
        parts.append((normed[...].astype(F32) * row[0] + row[1]).astype(BF16))
    modulated = jnp.concatenate(parts, 0)
    result = jnp.dot(modulated, weight[...], preferred_element_type=F32).astype(BF16)
    out[...] = result.reshape(out.shape)


def decode(mixed, w_mine, w_other, resid, gain, scale, shift, weight):
    count, rows = scale.shape[0], resid.shape[0]
    each = 2
    return pl.pallas_call(
        decode_kernel,
        grid=(count // each,),
        in_specs=[VMEM] * 7 + [HBM],
        out_specs=pl.BlockSpec((each, rows, D), lambda v: (v, 0, 0)),
        out_shape=shape((count, rows, D), BF16),
        scratch_shapes=[
            pltpu.VMEM((rows, D), BF16),
            pltpu.VMEM((D, D), BF16),
            pltpu.SemaphoreType.DMA(()),
        ],
        compiler_params=PARAMS,
        cost_estimate=cost(5<< 30, 8<< 20),
        name="decode",
    )(mixed, w_mine, w_other, resid, gain, scale, shift, weight)


def space_index(z, x, core):
    return (z * X + x) * CORES + core


def moves(step):
    return [
        (space_index(z, x, c), space_index(*step(z, x, c)))
        for z in range(Z_HI)
        for x in range(X)
        for c in range(CORES)
    ]


SWAP = moves(lambda z, x, c: (z, x, 1 - c))


def along_x(k):
    return moves(lambda z, x, c: (z, (x + k) % X, c))


def along_z(k):
    return moves(lambda z, x, c: ((z + k) % Z_HI, x, c))


def exchange(array):
    return lax.all_to_all(array, "chan", 0, 0, tiled=True)


def body(
    patches,
    var_embed,
    agg_query,
    pos_embed,
    gain_first,
    gain_second,
    w_qkv,
    w_out,
    w_dec,
    mod_scale,
    mod_shift,
):
    rows = patches.shape[1]
    peers = lax.axis_size("chan")

    parts = exchange(pool(patches, var_embed, agg_query.reshape(1, D), peers))
    resid = exchange(merge_pool(parts, pos_embed)).reshape(rows, D)

    mine, other, copies = project(
        resid, gain_first.reshape(1, D), w_qkv.transpose(1, 0, 2), w_out, peers
    )
    kv, qt = pair(mine, lax.ppermute(other, "space", SWAP))
    query_pieces = [qt] + [lax.ppermute(qt, "space", along_z(k)) for k in (2, 1, 3)]
    key_pieces = [kv] + [lax.ppermute(kv, "space", along_x(k)) for k in (2, 1, 3)]
    w_mine = exchange(copies)
    partial = attend(key_pieces, query_pieces)
    back = [partial[0]] + [
        lax.ppermute(p, "space", along_z(-k)) for p, k in zip(partial[1:], (2, 1, 3))
    ]
    mine, other = merge_heads(back, w_mine)
    w_other = lax.ppermute(w_mine, "space", SWAP)
    mixed = exchange(spread(mine, lax.ppermute(other, "space", SWAP), peers))
    gain = gain_second.reshape(1, D)
    return decode(mixed, w_mine, w_other, resid, gain, mod_scale, mod_shift, w_dec)


def solution(mesh):
    placed = (
        P("chan", "space", None),
        P("chan", None),
        P(),
        P("space", None),
        P(),
        P(),
        P(None, None, "chan"),
        P("chan", None),
        P(),
        P("chan", None),
        P("chan", None),
    )

    return jax.shard_map(
        body, mesh=mesh, in_specs=placed, out_specs=P("chan", "space", None), check_vma=False
    )
```

```python
import functools
import math

import jax
import jax.numpy as jnp
from jax import lax
from jax.experimental import pallas as pl
from jax.experimental.pallas import tpu as pltpu
from jax.sharding import PartitionSpec as P


D = 1024
HEADS = 16
HEAD_DIM = D // HEADS
EPS = 1e-6
LOG2E = 1.4426950408889634
Z_HI, X, CORES = 4, 4, 2
F32, BF16 = jnp.float32, jnp.bfloat16

VMEM = pl.BlockSpec(memory_space=pltpu.VMEM)
ANY = pl.BlockSpec(memory_space=pl.ANY)
PARAMS = pltpu.CompilerParams(vmem_limit_bytes=24 << 20)


def cost(flops, moved):
    return pl.CostEstimate(flops=flops, bytes_accessed=moved, transcendentals=0)


def shape(dims, dtype):
    return jax.ShapeDtypeStruct(dims, dtype)


def in_three(value):
    high = value.astype(BF16)
    rest = value - high.astype(F32)
    mid = rest.astype(BF16)
    low = (rest - mid.astype(F32)).astype(BF16)
    return high.astype(F32), mid.astype(F32), low.astype(F32)


def pool_kernel(patches, var_embed, query, out):
    count = patches.shape[0]
    parts, rows, _ = out.shape
    scaled = query[...] * (LOG2E / math.sqrt(D))
    shared = jnp.sum(var_embed[...] * scaled, -1, keepdims=True)
    lane = lax.broadcasted_iota(jnp.int32, (rows, 128), 1)
    for part in range(parts):
        here = slice(part * rows, (part + 1) * rows)
        logits = [
            jnp.sum(patches[v, here].astype(F32) * scaled, -1, keepdims=True) + shared[v : v + 1, :]
            for v in range(count)
        ]
        top = functools.reduce(jnp.maximum, logits)
        expo = [jnp.exp2(l - top) for l in logits]
        total = functools.reduce(jnp.add, expo)
        inverse = 1.0 / total
        acc = jnp.zeros((rows, D), F32)
        for v in range(count):
            embedded = patches[v, here].astype(F32) + var_embed[v : v + 1, :]
            acc = acc + (expo[v] * inverse) * embedded
        out[part, :, :D] = acc.astype(BF16)
        high, mid, low = in_three(top + jnp.log2(total))
        packed = jnp.where(lane == 0, high, jnp.where(lane == 1, mid, jnp.where(lane == 2, low, 0.0)))
        out[part, :, D:] = packed.astype(BF16)


def pool(patches, var_embed, query, peers):
    count, rows, _ = patches.shape
    part = rows // peers
    each = peers // 2
    return pl.pallas_call(
        pool_kernel,
        grid=(peers // each,),
        in_specs=[
            pl.BlockSpec((count, each * part, D), lambda i: (0, i, 0)),
            pl.BlockSpec((count, D), lambda i: (0, 0)),
            pl.BlockSpec((1, D), lambda i: (0, 0)),
        ],
        out_specs=pl.BlockSpec((each, part, D + 128), lambda i: (i, 0, 0)),
        out_shape=shape((peers, part, D + 128), BF16),
        cost_estimate=cost(16 << 20, 8 << 20),
        name="pool",
    )(patches, var_embed, query)


def merge_pool_kernel(parts, pos, resid):
    peers, rows, _ = parts.shape
    logs = [jnp.sum(parts[i, :, D:].astype(F32), -1, keepdims=True) for i in range(peers)]
    top = functools.reduce(jnp.maximum, logs)
    weights = [jnp.exp2(l - top) for l in logs]
    total = functools.reduce(jnp.add, weights)
    acc = jnp.zeros((rows, D), F32)
    for i in range(peers):
        acc = acc + (weights[i] / total) * parts[i, :, :D].astype(F32)
    start = pl.multiple_of(lax.axis_index("chan") * rows, rows)
    value = (acc + pos[pl.ds(start, rows), :].astype(F32)).astype(BF16)
    for i in range(peers):
        resid[i] = value


def merge_pool(parts, pos):
    peers, rows, _ = parts.shape
    return pl.pallas_call(
        merge_pool_kernel,
        in_specs=[VMEM, VMEM],
        out_specs=VMEM,
        out_shape=shape((peers, rows, D), BF16),
        compiler_params=PARAMS,
        cost_estimate=cost(4<< 20, 2<< 20),
        name="merge_pool",
    )(parts, pos)


def project_kernel(resid, gain, weight, w_out, mine, other, copies, sems):
    share = w_out.shape[0] // CORES
    start = pl.multiple_of(lax.axis_index("space") % CORES * share, share)
    source = w_out.at[pl.ds(start, share), :]
    moved = [pltpu.make_async_copy(source, copies.at[i], sems.at[i]) for i in range(copies.shape[0])]
    for copy in moved:
        copy.start()
    half = resid.shape[0] // 2
    value = resid[...].astype(F32)
    mean = jnp.mean(value * value, -1, keepdims=True)
    x = (value * lax.rsqrt(mean + EPS) * gain[...]).astype(BF16)
    q, k, v = (jnp.dot(x, weight[i], preferred_element_type=F32) for i in range(3))
    low = lax.broadcasted_iota(jnp.int32, (half, 2 * HEAD_DIM), 1) < HEAD_DIM
    upper, lower = k[:half], k[half:]
    keys = (
        jnp.where(low, upper, pltpu.roll(lower, HEAD_DIM, 1)),
        jnp.where(low, pltpu.roll(upper, HEAD_DIM, 1), lower),
    )
    turned = [(q * (1.0 / math.sqrt(HEAD_DIM))).T, v.T]
    queries, values = ((t[:HEAD_DIM], t[HEAD_DIM:]) for t in turned)
    is_first = lax.axis_index("space") % CORES == 0
    for ref, (a, b) in ((mine, (0, 1)), (other, (1, 0))):
        key, value, query = (
            jnp.where(is_first, pair[a], pair[b]).astype(BF16) for pair in (keys, values, queries)
        )
        ref[:half, :] = key
        for i, turn in ((1, value), (2, query)):
            ref[i * half : i * half + HEAD_DIM, :] = turn[:, :half]
            ref[i * half + HEAD_DIM : (i + 1) * half, :] = turn[:, half:]
    for copy in moved:
        copy.wait()


def project(resid, gain, weight, w_out, peers):
    out = shape((resid.shape[0] + 2 * HEAD_DIM, 128), BF16)
    return pl.pallas_call(
        project_kernel,
        in_specs=[VMEM] * 4,
        out_specs=(VMEM, VMEM, ANY),
        out_shape=(out, out, shape((peers, w_out.shape[0] // CORES, D), BF16)),
        scratch_shapes=[pltpu.SemaphoreType.DMA((peers,))],
        compiler_params=PARAMS,
        cost_estimate=cost(200 << 20, 4<< 20),
        name="project",
    )(resid, gain, weight, w_out)


def pair_kernel(mine, swapped, kv, qt):
    rows, turned = kv.shape[0] // 2, qt.shape[0] // 2
    kv[:rows, :] = mine[:rows, :]
    kv[rows:, :] = swapped[:rows, :]
    qt[:turned, :] = mine[rows:, :]
    qt[turned:, :] = swapped[rows:, :]


def pair(mine, swapped):
    rows = mine.shape[0] - 2 * HEAD_DIM
    return pl.pallas_call(
        pair_kernel,
        in_specs=[VMEM, VMEM],
        out_specs=(VMEM, VMEM),
        out_shape=(shape((2 * rows, 128), BF16), shape((4 * HEAD_DIM, 128), BF16)),
        compiler_params=PARAMS,
        cost_estimate=cost(1<< 20, 1<< 20),
        name="pair",
    )(mine, swapped)


def attend_kernel(k0, k1, k2, k3, queries, out):
    zeros = jnp.zeros((HEAD_DIM, 256), BF16)
    groups = ((k0, k1), (k2, k3))

    def scores_of(tile, refs):
        at = tile * 2 * HEAD_DIM
        turned = jnp.concatenate(
            [queries[at : at + HEAD_DIM, :], queries[at + HEAD_DIM : at + 2 * HEAD_DIM, :]], 1
        )
        sides = jnp.concatenate([turned, zeros], 0), jnp.concatenate([zeros, turned], 0)
        return [
            jnp.dot(ref[at : at + 128, :], side, preferred_element_type=F32)
            for ref in refs
            for at in (0, 256)
            for side in sides
        ]

    def merged(state, scores, refs):
        top = functools.reduce(jnp.maximum, [jnp.max(s, 0, keepdims=True) for s in scores]) * LOG2E
        if state is not None:
            top = jnp.maximum(state[0], top)
        probs = [jnp.exp2(s * LOG2E - top) for s in scores]
        total = functools.reduce(jnp.add, [jnp.sum(p, 0, keepdims=True) for p in probs])
        values = [
            jnp.concatenate([ref[at + 128 : at + 192, :], ref[at + 192 : at + 256, :]], 1)
            for ref in refs
            for at in (0, 256)
        ]
        acc = jnp.zeros((HEAD_DIM, 256), F32)
        for i, value in enumerate(values):
            pair = jnp.concatenate([p.astype(BF16) for p in probs[2 * i : 2 * i + 2]], 0)
            acc += jnp.dot(value, pair, preferred_element_type=F32)
        if state is not None:
            rescale = jnp.exp2(state[0] - top)
            total = total + rescale * state[1]
            acc = acc + rescale * state[2]
        return top, total, acc

    work = [(tile, refs) for refs in groups for tile in range(2)]
    states = [None, None]
    ahead = scores_of(*work[0])
    for i, (tile, refs) in enumerate(work):
        scores = ahead
        if i + 1 < len(work):
            ahead = scores_of(*work[i + 1])
        states[tile] = merged(states[tile], scores, refs)
    for tile, (top, total, acc) in enumerate(states):
        lanes = slice(tile * 256, tile * 256 + 256)
        out[:HEAD_DIM, lanes] = (acc / total).astype(BF16)
        high, mid, low = in_three(top + jnp.log2(total))
        row = lax.broadcasted_iota(jnp.int32, (16, 256), 0)
        logs = jnp.where(row == 0, high, jnp.where(row == 1, mid, jnp.where(row == 2, low, 0.0)))
        out[HEAD_DIM:, lanes] = logs.astype(BF16)


def attend(key_pieces, queries):
    each = key_pieces[0].shape[0]
    return pl.pallas_call(
        attend_kernel,
        in_specs=[VMEM] * 5,
        out_specs=VMEM,
        out_shape=shape((HEAD_DIM + 16, each), BF16),
        compiler_params=PARAMS,
        cost_estimate=cost(1 << 30, 2 << 20),
        name="attend",
    )(*key_pieces, queries)


def merge_heads_kernel(p0, p1, p2, p3, mine, other):
    refs = (p0, p1, p2, p3)
    logs = [jnp.sum(r[HEAD_DIM:, :].astype(F32), 0, keepdims=True) for r in refs]
    top = functools.reduce(jnp.maximum, logs)
    weights = [jnp.exp2(l - top) for l in logs]
    total = functools.reduce(jnp.add, weights)
    acc = jnp.zeros((HEAD_DIM, p0.shape[1]), F32)
    for r, w in zip(refs, weights):
        acc = acc + (w / total) * r[:HEAD_DIM, :].astype(F32)
    half = p0.shape[1] // 2
    mine[...] = acc[:, :half].astype(BF16)
    other[...] = acc[:, half:].astype(BF16)


def merge_heads(parts):
    width = parts[0].shape[1] // 2
    out = shape((HEAD_DIM, width), BF16)
    return pl.pallas_call(
        merge_heads_kernel,
        in_specs=[VMEM] * 4,
        out_specs=(VMEM, VMEM),
        out_shape=(out, out),
        compiler_params=PARAMS,
        cost_estimate=cost(1<< 20, 1<< 20),
        name="merge_heads",
    )(*parts)


def spread_kernel(mine, other, _, out):
    both = jnp.concatenate([mine[...].astype(F32), other[...].astype(F32)], 0)
    value = both.T.astype(BF16)
    for i in range(out.shape[0]):
        out[i] = value


def spread(mine, other, after, peers):
    return pl.pallas_call(
        spread_kernel,
        in_specs=[VMEM, VMEM, ANY],
        out_specs=VMEM,
        out_shape=shape((peers, mine.shape[1], 2 * HEAD_DIM), BF16),
        compiler_params=PARAMS,
        cost_estimate=cost(1<< 20, 1<< 20),
        name="spread",
    )(mine, other, after)


def trunk_kernel(mixed, w_mine, w_other, resid, gain, normed):
    heads = jnp.concatenate([mixed[i] for i in range(mixed.shape[0])], 1)
    weights = [ref[i] for i in range(mixed.shape[0]) for ref in (w_mine, w_other)]
    value = jnp.dot(heads, jnp.concatenate(weights, 0), preferred_element_type=F32)
    value = value + resid[...].astype(F32)
    mean = jnp.mean(value * value, -1, keepdims=True)
    normed[...] = (value * lax.rsqrt(mean + EPS) * gain[...]).astype(BF16)


def trunk(mixed, w_mine, w_other, resid, gain):
    return pl.pallas_call(
        trunk_kernel,
        in_specs=[VMEM] * 5,
        out_specs=VMEM,
        out_shape=shape(resid.shape, BF16),
        compiler_params=PARAMS,
        cost_estimate=cost(1 << 30, 4 << 20),
        name="trunk",
    )(mixed, w_mine, w_other, resid, gain)


def decode_kernel(normed, scale, shift, weight, out):
    each = out.shape[0]
    parts = []
    for i in range(each):
        v = pl.program_id(0) * each + i
        row = (1.0 + scale[pl.ds(v, 1), :], shift[pl.ds(v, 1), :])
        parts.append((normed[...].astype(F32) * row[0] + row[1]).astype(BF16))
    modulated = jnp.concatenate(parts, 0)
    result = jnp.dot(modulated, weight[...], preferred_element_type=F32).astype(BF16)
    out[...] = result.reshape(out.shape)


def decode(normed, scale, shift, weight):
    count, rows = scale.shape[0], normed.shape[0]
    each = 2
    return pl.pallas_call(
        decode_kernel,
        grid=(count // each,),
        in_specs=[VMEM] * 4,
        out_specs=pl.BlockSpec((each, rows, D), lambda v: (v, 0, 0)),
        out_shape=shape((count, rows, D), BF16),
        compiler_params=PARAMS,
        cost_estimate=cost(5 << 30, 8 << 20),
        name="decode",
    )(normed, scale, shift, weight)


def space_index(z, x, core):
    return (z * X + x) * CORES + core


def moves(step):
    return [
        (space_index(z, x, c), space_index(*step(z, x, c)))
        for z in range(Z_HI)
        for x in range(X)
        for c in range(CORES)
    ]


SWAP = moves(lambda z, x, c: (z, x, 1 - c))


def along_x(k):
    return moves(lambda z, x, c: (z, (x + k) % X, c))


def along_z(k):
    return moves(lambda z, x, c: ((z + k) % Z_HI, x, c))


def exchange(array):
    return lax.all_to_all(array, "chan", 0, 0, tiled=True)


def body(
    patches,
    var_embed,
    agg_query,
    pos_embed,
    gain_first,
    gain_second,
    w_qkv,
    w_out,
    w_dec,
    mod_scale,
    mod_shift,
):
    rows = patches.shape[1]
    peers = lax.axis_size("chan")

    parts = exchange(pool(patches, var_embed, agg_query.reshape(1, D), peers))
    resid = exchange(merge_pool(parts, pos_embed)).reshape(rows, D)

    mine, other, copies = project(
        resid, gain_first.reshape(1, D), w_qkv.transpose(1, 0, 2), w_out, peers
    )
    kv, qt = pair(mine, lax.ppermute(other, "space", SWAP))
    key_pieces = [kv] + [lax.ppermute(kv, "space", along_z(k)) for k in (2, 1, 3)]
    query_pieces = [lax.ppermute(qt, "space", along_x(k)) for k in (2, 1, 3)]
    w_mine = exchange(copies)
    back = []
    for k, piece in zip((2, 1, 3), query_pieces):
        partial = attend(key_pieces, piece)
        back.append(lax.ppermute(partial, "space", along_x(-k)))
    back.append(attend(key_pieces, qt))
    mine, other = merge_heads(back)
    w_other = lax.ppermute(w_mine, "space", SWAP)
    mixed = exchange(spread(mine, lax.ppermute(other, "space", SWAP), w_mine, peers))
    normed = trunk(mixed, w_mine, w_other, resid, gain_second.reshape(1, D))
    return decode(normed, mod_scale, mod_shift, w_dec)


def solution(mesh):
    placed = (
        P("chan", "space", None),
        P("chan", None),
        P(),
        P("space", None),
        P(),
        P(),
        P(None, None, "chan"),
        P("chan", None),
        P(),
        P("chan", None),
        P("chan", None),
    )

    return jax.shard_map(
        body, mesh=mesh, in_specs=placed, out_specs=P("chan", "space", None), check_vma=False
    )
```

```python
import functools
import math

import jax
import jax.numpy as jnp
from jax import lax
from jax.experimental import pallas as pl
from jax.experimental.pallas import tpu as pltpu
from jax.sharding import PartitionSpec as P


D = 1024
HEADS = 16
HEAD_DIM = D // HEADS
EPS = 1e-6
LOG2E = 1.4426950408889634
Z_HI, X, CORES = 4, 4, 2
F32, BF16 = jnp.float32, jnp.bfloat16

VMEM = pl.BlockSpec(memory_space=pltpu.VMEM)
ANY = pl.BlockSpec(memory_space=pl.ANY)
PARAMS = pltpu.CompilerParams(vmem_limit_bytes=24 << 20)


def cost(flops, moved):
    return pl.CostEstimate(flops=flops, bytes_accessed=moved, transcendentals=0)


def shape(dims, dtype):
    return jax.ShapeDtypeStruct(dims, dtype)


def in_three(value):
    high = value.astype(BF16)
    rest = value - high.astype(F32)
    mid = rest.astype(BF16)
    low = (rest - mid.astype(F32)).astype(BF16)
    return high.astype(F32), mid.astype(F32), low.astype(F32)


def pool_kernel(patches, var_embed, query, out):
    count = patches.shape[0]
    parts, rows, _ = out.shape
    scaled = query[...] * (LOG2E / math.sqrt(D))
    shared = jnp.sum(var_embed[...] * scaled, -1, keepdims=True)
    lane = lax.broadcasted_iota(jnp.int32, (rows, 128), 1)
    for part in range(parts):
        here = slice(part * rows, (part + 1) * rows)
        logits = [
            jnp.sum(patches[v, here].astype(F32) * scaled, -1, keepdims=True) + shared[v : v + 1, :]
            for v in range(count)
        ]
        top = functools.reduce(jnp.maximum, logits)
        expo = [jnp.exp2(l - top) for l in logits]
        total = functools.reduce(jnp.add, expo)
        inverse = 1.0 / total
        acc = jnp.zeros((rows, D), F32)
        for v in range(count):
            embedded = patches[v, here].astype(F32) + var_embed[v : v + 1, :]
            acc = acc + (expo[v] * inverse) * embedded
        out[part, :, :D] = acc.astype(BF16)
        high, mid, low = in_three(top + jnp.log2(total))
        packed = jnp.where(lane == 0, high, jnp.where(lane == 1, mid, jnp.where(lane == 2, low, 0.0)))
        out[part, :, D:] = packed.astype(BF16)


def pool(patches, var_embed, query, peers):
    count, rows, _ = patches.shape
    part = rows // peers
    each = peers // 2
    return pl.pallas_call(
        pool_kernel,
        grid=(peers // each,),
        in_specs=[
            pl.BlockSpec((count, each * part, D), lambda i: (0, i, 0)),
            pl.BlockSpec((count, D), lambda i: (0, 0)),
            pl.BlockSpec((1, D), lambda i: (0, 0)),
        ],
        out_specs=pl.BlockSpec((each, part, D + 128), lambda i: (i, 0, 0)),
        out_shape=shape((peers, part, D + 128), BF16),
        cost_estimate=cost(16 << 20, 8 << 20),
        name="pool",
    )(patches, var_embed, query)


def merge_pool_kernel(parts, pos, resid):
    peers, rows, _ = parts.shape
    logs = [jnp.sum(parts[i, :, D:].astype(F32), -1, keepdims=True) for i in range(peers)]
    top = functools.reduce(jnp.maximum, logs)
    weights = [jnp.exp2(l - top) for l in logs]
    total = functools.reduce(jnp.add, weights)
    acc = jnp.zeros((rows, D), F32)
    for i in range(peers):
        acc = acc + (weights[i] / total) * parts[i, :, :D].astype(F32)
    start = pl.multiple_of(lax.axis_index("chan") * rows, rows)
    value = (acc + pos[pl.ds(start, rows), :].astype(F32)).astype(BF16)
    for i in range(peers):
        resid[i] = value


def merge_pool(parts, pos):
    peers, rows, _ = parts.shape
    return pl.pallas_call(
        merge_pool_kernel,
        in_specs=[VMEM, VMEM],
        out_specs=VMEM,
        out_shape=shape((peers, rows, D), BF16),
        compiler_params=PARAMS,
        cost_estimate=cost(4<< 20, 2<< 20),
        name="merge_pool",
    )(parts, pos)


def project_kernel(resid, gain, weight, w_out, kv, qt, copies, sems):
    share = w_out.shape[0] // CORES
    start = pl.multiple_of(lax.axis_index("space") % CORES * share, share)
    source = w_out.at[pl.ds(start, share), :]
    moved = [pltpu.make_async_copy(source, copies.at[i], sems.at[i]) for i in range(copies.shape[0])]
    for copy in moved:
        copy.start()
    half = resid.shape[0] // 2
    value = resid[...].astype(F32)
    mean = jnp.mean(value * value, -1, keepdims=True)
    x = (value * lax.rsqrt(mean + EPS) * gain[...]).astype(BF16)
    q, k, v = (jnp.dot(x, weight[i], preferred_element_type=F32) for i in range(3))
    low = lax.broadcasted_iota(jnp.int32, (half, 2 * HEAD_DIM), 1) < HEAD_DIM
    upper, lower = k[:half], k[half:]
    kv[:half, :] = jnp.where(low, upper, pltpu.roll(lower, HEAD_DIM, 1)).astype(BF16)
    kv[2 * half : 3 * half, :] = jnp.where(low, pltpu.roll(upper, HEAD_DIM, 1), lower).astype(BF16)
    queries = (q * (1.0 / math.sqrt(HEAD_DIM))).T.astype(BF16)
    values = v.T.astype(BF16)
    for head in range(2):
        for side in range(2):
            piece = slice(head * HEAD_DIM, (head + 1) * HEAD_DIM), slice(side * half, (side + 1) * half)
            at = (2 * head + 1) * half + side * HEAD_DIM
            kv[at : at + HEAD_DIM, :] = values[piece]
            at = head * half + side * HEAD_DIM
            qt[at : at + HEAD_DIM, :] = queries[piece]
    for copy in moved:
        copy.wait()


def project(resid, gain, weight, w_out, peers):
    rows = resid.shape[0]
    return pl.pallas_call(
        project_kernel,
        in_specs=[VMEM] * 4,
        out_specs=(VMEM, VMEM, ANY),
        out_shape=(
            shape((2 * rows, 128), BF16),
            shape((rows, 128), BF16),
            shape((peers, w_out.shape[0] // CORES, D), BF16),
        ),
        scratch_shapes=[pltpu.SemaphoreType.DMA((peers,))],
        compiler_params=PARAMS,
        cost_estimate=cost(200 << 20, 4 << 20),
        name="project",
    )(resid, gain, weight, w_out)


def attend_kernel(*args):
    *pieces, queries, out = args
    zeros = jnp.zeros((HEAD_DIM, 256), BF16)
    groups = (pieces[:4], pieces[4:])

    def scores_of(tile, refs):
        at = tile * 2 * HEAD_DIM
        turned = jnp.concatenate(
            [queries[at : at + HEAD_DIM, :], queries[at + HEAD_DIM : at + 2 * HEAD_DIM, :]], 1
        )
        sides = jnp.concatenate([turned, zeros], 0), jnp.concatenate([zeros, turned], 0)
        return [
            jnp.dot(ref[tile * 256 : tile * 256 + 128, :], side, preferred_element_type=F32)
            for ref in refs
            for side in sides
        ]

    def merged(state, scores, tile, refs):
        top = functools.reduce(jnp.maximum, [jnp.max(s, 0, keepdims=True) for s in scores]) * LOG2E
        if state is not None:
            top = jnp.maximum(state[0], top)
        probs = [jnp.exp2(s * LOG2E - top) for s in scores]
        total = functools.reduce(jnp.add, [jnp.sum(p, 0, keepdims=True) for p in probs])
        values = [
            jnp.concatenate([ref[at : at + HEAD_DIM, :], ref[at + HEAD_DIM : at + 2 * HEAD_DIM, :]], 1)
            for ref in refs
            for at in (tile * 256 + 128,)
        ]
        acc = jnp.zeros((HEAD_DIM, 256), F32)
        for i, value in enumerate(values):
            pair = jnp.concatenate([p.astype(BF16) for p in probs[2 * i : 2 * i + 2]], 0)
            acc += jnp.dot(value, pair, preferred_element_type=F32)
        if state is not None:
            rescale = jnp.exp2(state[0] - top)
            total = total + rescale * state[1]
            acc = acc + rescale * state[2]
        return top, total, acc

    work = [(tile, refs) for refs in groups for tile in range(2)]
    states = [None, None]
    ahead = scores_of(*work[0])
    for i, (tile, refs) in enumerate(work):
        scores = ahead
        if i + 1 < len(work):
            ahead = scores_of(*work[i + 1])
        states[tile] = merged(states[tile], scores, tile, refs)
    for tile, (top, total, acc) in enumerate(states):
        lanes = slice(tile * 256, tile * 256 + 256)
        out[:HEAD_DIM, lanes] = (acc / total).astype(BF16)
        high, mid, low = in_three(top + jnp.log2(total))
        row = lax.broadcasted_iota(jnp.int32, (16, 256), 0)
        logs = jnp.where(row == 0, high, jnp.where(row == 1, mid, jnp.where(row == 2, low, 0.0)))
        out[HEAD_DIM:, lanes] = logs.astype(BF16)


def attend(key_pieces, queries):
    each = key_pieces[0].shape[0]
    return pl.pallas_call(
        attend_kernel,
        in_specs=[VMEM] * 9,
        out_specs=VMEM,
        out_shape=shape((HEAD_DIM + 16, each), BF16),
        compiler_params=PARAMS,
        cost_estimate=cost(1 << 30, 2 << 20),
        name="attend",
    )(*key_pieces, queries)


def merge_heads_kernel(p0, p1, p2, p3, out):
    refs = (p0, p1, p2, p3)
    logs = [jnp.sum(r[HEAD_DIM:, :].astype(F32), 0, keepdims=True) for r in refs]
    top = functools.reduce(jnp.maximum, logs)
    weights = [jnp.exp2(l - top) for l in logs]
    total = functools.reduce(jnp.add, weights)
    acc = jnp.zeros((HEAD_DIM, p0.shape[1]), F32)
    for r, w in zip(refs, weights):
        acc = acc + (w / total) * r[:HEAD_DIM, :].astype(F32)
    half = p0.shape[1] // 2
    is_first = lax.axis_index("space") % CORES == 0
    a, b = acc[:, :half], acc[:, half:]
    out[:HEAD_DIM, :] = jnp.where(is_first, a, b)
    out[HEAD_DIM:, :] = jnp.where(is_first, b, a)


def merge_heads(parts):
    return pl.pallas_call(
        merge_heads_kernel,
        in_specs=[VMEM] * 4,
        out_specs=VMEM,
        out_shape=shape((2 * HEAD_DIM, parts[0].shape[1] // 2), F32),
        compiler_params=PARAMS,
        cost_estimate=cost(1 << 20, 1 << 20),
        name="merge_heads",
    )(*parts)


def spread_kernel(both, _, out):
    value = both[...].T.astype(BF16)
    for i in range(out.shape[0]):
        out[i] = value


def spread(both, after, peers):
    return pl.pallas_call(
        spread_kernel,
        in_specs=[VMEM, ANY],
        out_specs=VMEM,
        out_shape=shape((peers, both.shape[1], both.shape[0]), BF16),
        compiler_params=PARAMS,
        cost_estimate=cost(1 << 20, 1 << 20),
        name="spread",
    )(both, after)


def trunk_kernel(mixed, w_mine, w_other, resid, gain, normed):
    heads = jnp.concatenate([mixed[i] for i in range(mixed.shape[0])], 1)
    weights = [ref[i] for i in range(mixed.shape[0]) for ref in (w_mine, w_other)]
    value = jnp.dot(heads, jnp.concatenate(weights, 0), preferred_element_type=F32)
    value = value + resid[...].astype(F32)
    mean = jnp.mean(value * value, -1, keepdims=True)
    normed[...] = (value * lax.rsqrt(mean + EPS) * gain[...]).astype(BF16)


def trunk(mixed, w_mine, w_other, resid, gain):
    return pl.pallas_call(
        trunk_kernel,
        in_specs=[VMEM] * 5,
        out_specs=VMEM,
        out_shape=shape(resid.shape, BF16),
        compiler_params=PARAMS,
        cost_estimate=cost(1 << 30, 4 << 20),
        name="trunk",
    )(mixed, w_mine, w_other, resid, gain)


def decode_kernel(normed, scale, shift, weight, out):
    each = out.shape[0]
    parts = []
    for i in range(each):
        v = pl.program_id(0) * each + i
        row = (1.0 + scale[pl.ds(v, 1), :], shift[pl.ds(v, 1), :])
        parts.append((normed[...].astype(F32) * row[0] + row[1]).astype(BF16))
    modulated = jnp.concatenate(parts, 0)
    result = jnp.dot(modulated, weight[...], preferred_element_type=F32).astype(BF16)
    out[...] = result.reshape(out.shape)


def decode(normed, scale, shift, weight):
    count, rows = scale.shape[0], normed.shape[0]
    each = 2
    return pl.pallas_call(
        decode_kernel,
        grid=(count // each,),
        in_specs=[VMEM] * 4,
        out_specs=pl.BlockSpec((each, rows, D), lambda v: (v, 0, 0)),
        out_shape=shape((count, rows, D), BF16),
        compiler_params=PARAMS,
        cost_estimate=cost(5 << 30, 8 << 20),
        name="decode",
    )(normed, scale, shift, weight)


def space_index(z, x, core):
    return (z * X + x) * CORES + core


def moves(step):
    return [
        (space_index(z, x, c), space_index(*step(z, x, c)))
        for z in range(Z_HI)
        for x in range(X)
        for c in range(CORES)
    ]


SWAP = moves(lambda z, x, c: (z, x, 1 - c))


def along_x(k):
    return moves(lambda z, x, c: (z, (x + k) % X, c))


def along_z(k):
    return moves(lambda z, x, c: ((z + k) % Z_HI, x, c))


def exchange(array):
    return lax.all_to_all(array, "chan", 0, 0, tiled=True)


def body(
    patches,
    var_embed,
    agg_query,
    pos_embed,
    gain_first,
    gain_second,
    w_qkv,
    w_out,
    w_dec,
    mod_scale,
    mod_shift,
):
    rows = patches.shape[1]
    peers = lax.axis_size("chan")

    parts = exchange(pool(patches, var_embed, agg_query.reshape(1, D), peers))
    resid = exchange(merge_pool(parts, pos_embed)).reshape(rows, D)

    kv, qt, copies = project(
        resid, gain_first.reshape(1, D), w_qkv.transpose(1, 0, 2), w_out, peers
    )
    key_pieces = [lax.ppermute(kv, "space", along_z(k)) for k in (2, 1, 3)]
    query_pieces = [lax.ppermute(qt, "space", along_x(k)) for k in (2, 1, 3)]
    w_mine = exchange(copies)
    key_pieces = [kv] + key_pieces
    key_pieces = key_pieces + [lax.ppermute(k, "space", SWAP) for k in key_pieces]
    back = []
    for k, piece in zip((2, 1, 3), query_pieces):
        partial = attend(key_pieces, piece)
        back.append(lax.ppermute(partial, "space", along_x(-k)))
    back.append(attend(key_pieces, qt))
    both = merge_heads(back)
    mixed = exchange(spread(both, w_mine, peers))
    w_other = lax.ppermute(w_mine, "space", SWAP)
    normed = trunk(mixed, w_mine, w_other, resid, gain_second.reshape(1, D))
    return decode(normed, mod_scale, mod_shift, w_dec)


def solution(mesh):
    placed = (
        P("chan", "space", None),
        P("chan", None),
        P(),
        P("space", None),
        P(),
        P(),
        P(None, None, "chan"),
        P("chan", None),
        P(),
        P("chan", None),
        P("chan", None),
    )

    return jax.shard_map(
        body, mesh=mesh, in_specs=placed, out_specs=P("chan", "space", None), check_vma=False
    )
```

```python
import functools
import math

import jax
import jax.numpy as jnp
from jax import lax
from jax.experimental import pallas as pl
from jax.experimental.pallas import tpu as pltpu
from jax.sharding import PartitionSpec as P


D = 1024
HEADS = 16
HEAD_DIM = D // HEADS
EPS = 1e-6
LOG2E = 1.4426950408889634
Z_HI, X, CORES = 4, 4, 2
F32, BF16 = jnp.float32, jnp.bfloat16

VMEM = pl.BlockSpec(memory_space=pltpu.VMEM)
ANY = pl.BlockSpec(memory_space=pl.ANY)
PARAMS = pltpu.CompilerParams(vmem_limit_bytes=24 << 20)


def cost(flops, moved):
    return pl.CostEstimate(flops=flops, bytes_accessed=moved, transcendentals=0)


def shape(dims, dtype):
    return jax.ShapeDtypeStruct(dims, dtype)


def in_three(value):
    high = value.astype(BF16)
    rest = value - high.astype(F32)
    mid = rest.astype(BF16)
    low = (rest - mid.astype(F32)).astype(BF16)
    return high.astype(F32), mid.astype(F32), low.astype(F32)


def pool_kernel(patches, var_embed, query, out):
    count = patches.shape[0]
    rows = out.shape[1]
    parts = patches.shape[1] // rows
    first = pl.program_id(0) * parts
    scaled = query[...] * (LOG2E / math.sqrt(D))
    shared = jnp.sum(var_embed[...] * scaled, -1, keepdims=True)
    lane = lax.broadcasted_iota(jnp.int32, (rows, 128), 1)
    for part in range(parts):
        here = slice(part * rows, (part + 1) * rows)
        logits = [
            jnp.sum(patches[v, here].astype(F32) * scaled, -1, keepdims=True) + shared[v : v + 1, :]
            for v in range(count)
        ]
        top = functools.reduce(jnp.maximum, logits)
        expo = [jnp.exp2(l - top) for l in logits]
        total = functools.reduce(jnp.add, expo)
        inverse = 1.0 / total
        acc = jnp.zeros((rows, D), F32)
        for v in range(count):
            embedded = patches[v, here].astype(F32) + var_embed[v : v + 1, :]
            acc = acc + (expo[v] * inverse) * embedded
        out[first + part, :, :D] = acc.astype(BF16)
        high, mid, low = in_three(top + jnp.log2(total))
        packed = jnp.where(lane == 0, high, jnp.where(lane == 1, mid, jnp.where(lane == 2, low, 0.0)))
        out[first + part, :, D:] = packed.astype(BF16)


def pool(patches, var_embed, query, peers):
    count, rows, _ = patches.shape
    part = rows // peers
    each = peers // 2
    return pl.pallas_call(
        pool_kernel,
        grid=(peers // each,),
        in_specs=[
            pl.BlockSpec((count, each * part, D), lambda i: (0, i, 0)),
            pl.BlockSpec((count, D), lambda i: (0, 0)),
            pl.BlockSpec((1, D), lambda i: (0, 0)),
        ],
        out_specs=VMEM,
        out_shape=shape((peers, part, D + 128), BF16),
        compiler_params=pltpu.CompilerParams(vmem_limit_bytes=52 << 20),
        cost_estimate=cost(16 << 20, 8 << 20),
        name="pool",
    )(patches, var_embed, query)


def merge_pool_kernel(parts, pos, resid):
    peers, rows, _ = parts.shape
    logs = [jnp.sum(parts[i, :, D:].astype(F32), -1, keepdims=True) for i in range(peers)]
    top = functools.reduce(jnp.maximum, logs)
    weights = [jnp.exp2(l - top) for l in logs]
    total = functools.reduce(jnp.add, weights)
    acc = jnp.zeros((rows, D), F32)
    for i in range(peers):
        acc = acc + (weights[i] / total) * parts[i, :, :D].astype(F32)
    start = pl.multiple_of(lax.axis_index("chan") * rows, rows)
    value = (acc + pos[pl.ds(start, rows), :].astype(F32)).astype(BF16)
    for i in range(peers):
        resid[i] = value


def merge_pool(parts, pos):
    peers, rows, _ = parts.shape
    return pl.pallas_call(
        merge_pool_kernel,
        in_specs=[VMEM, VMEM],
        out_specs=VMEM,
        out_shape=shape((peers, rows, D), BF16),
        compiler_params=PARAMS,
        cost_estimate=cost(4<< 20, 2<< 20),
        name="merge_pool",
    )(parts, pos)


def project_kernel(resid, gain, weight, w_out, kv, qt, copies, sems):
    share = w_out.shape[0] // CORES
    start = pl.multiple_of(lax.axis_index("space") % CORES * share, share)
    source = w_out.at[pl.ds(start, share), :]
    moved = [pltpu.make_async_copy(source, copies.at[i], sems.at[i]) for i in range(copies.shape[0])]
    for copy in moved:
        copy.start()
    half = resid.shape[0] // 2
    value = resid[...].astype(F32)
    mean = jnp.mean(value * value, -1, keepdims=True)
    x = (value * lax.rsqrt(mean + EPS) * gain[...]).astype(BF16)
    q, k, v = (jnp.dot(x, weight[i], preferred_element_type=F32) for i in range(3))
    low = lax.broadcasted_iota(jnp.int32, (half, 2 * HEAD_DIM), 1) < HEAD_DIM
    upper, lower = k[:half], k[half:]
    kv[:half, :] = jnp.where(low, upper, pltpu.roll(lower, HEAD_DIM, 1)).astype(BF16)
    kv[2 * half : 3 * half, :] = jnp.where(low, pltpu.roll(upper, HEAD_DIM, 1), lower).astype(BF16)
    queries = (q * (1.0 / math.sqrt(HEAD_DIM))).T.astype(BF16)
    values = v.T.astype(BF16)
    for head in range(2):
        for side in range(2):
            piece = slice(head * HEAD_DIM, (head + 1) * HEAD_DIM), slice(side * half, (side + 1) * half)
            at = (2 * head + 1) * half + side * HEAD_DIM
            kv[at : at + HEAD_DIM, :] = values[piece]
            at = head * half + side * HEAD_DIM
            qt[at : at + HEAD_DIM, :] = queries[piece]
    for copy in moved:
        copy.wait()


def project(resid, gain, weight, w_out, peers):
    rows = resid.shape[0]
    return pl.pallas_call(
        project_kernel,
        in_specs=[VMEM] * 4,
        out_specs=(VMEM, VMEM, ANY),
        out_shape=(
            shape((2 * rows, 128), BF16),
            shape((rows, 128), BF16),
            shape((peers, w_out.shape[0] // CORES, D), BF16),
        ),
        scratch_shapes=[pltpu.SemaphoreType.DMA((peers,))],
        compiler_params=PARAMS,
        cost_estimate=cost(200 << 20, 4 << 20),
        name="project",
    )(resid, gain, weight, w_out)


def attend_kernel(*args):
    *pieces, queries, out = args
    zeros = jnp.zeros((HEAD_DIM, 256), BF16)
    groups = (pieces[:4], pieces[4:])

    def scores_of(tile, refs):
        at = tile * 2 * HEAD_DIM
        turned = jnp.concatenate(
            [queries[at : at + HEAD_DIM, :], queries[at + HEAD_DIM : at + 2 * HEAD_DIM, :]], 1
        )
        sides = jnp.concatenate([turned, zeros], 0), jnp.concatenate([zeros, turned], 0)
        return [
            jnp.dot(ref[tile * 256 : tile * 256 + 128, :], side, preferred_element_type=F32)
            for ref in refs
            for side in sides
        ]

    def merged(state, scores, tile, refs):
        top = functools.reduce(jnp.maximum, [jnp.max(s, 0, keepdims=True) for s in scores]) * LOG2E
        if state is not None:
            top = jnp.maximum(state[0], top)
        probs = [jnp.exp2(s * LOG2E - top) for s in scores]
        total = functools.reduce(jnp.add, [jnp.sum(p, 0, keepdims=True) for p in probs])
        values = [
            jnp.concatenate([ref[at : at + HEAD_DIM, :], ref[at + HEAD_DIM : at + 2 * HEAD_DIM, :]], 1)
            for ref in refs
            for at in (tile * 256 + 128,)
        ]
        acc = jnp.zeros((HEAD_DIM, 256), F32)
        for i, value in enumerate(values):
            pair = jnp.concatenate([p.astype(BF16) for p in probs[2 * i : 2 * i + 2]], 0)
            acc += jnp.dot(value, pair, preferred_element_type=F32)
        if state is not None:
            rescale = jnp.exp2(state[0] - top)
            total = total + rescale * state[1]
            acc = acc + rescale * state[2]
        return top, total, acc

    work = [(tile, refs) for refs in groups for tile in range(2)]
    states = [None, None]
    ahead = scores_of(*work[0])
    for i, (tile, refs) in enumerate(work):
        scores = ahead
        if i + 1 < len(work):
            ahead = scores_of(*work[i + 1])
        states[tile] = merged(states[tile], scores, tile, refs)
    for tile, (top, total, acc) in enumerate(states):
        lanes = slice(tile * 256, tile * 256 + 256)
        out[:HEAD_DIM, lanes] = (acc / total).astype(BF16)
        high, mid, low = in_three(top + jnp.log2(total))
        row = lax.broadcasted_iota(jnp.int32, (16, 256), 0)
        logs = jnp.where(row == 0, high, jnp.where(row == 1, mid, jnp.where(row == 2, low, 0.0)))
        out[HEAD_DIM:, lanes] = logs.astype(BF16)


def attend(key_pieces, queries):
    each = key_pieces[0].shape[0]
    return pl.pallas_call(
        attend_kernel,
        in_specs=[VMEM] * 9,
        out_specs=VMEM,
        out_shape=shape((HEAD_DIM + 16, each), BF16),
        compiler_params=PARAMS,
        cost_estimate=cost(1 << 30, 2 << 20),
        name="attend",
    )(*key_pieces, queries)


def merge_heads_kernel(p0, p1, p2, p3, out):
    refs = (p0, p1, p2, p3)
    logs = [jnp.sum(r[HEAD_DIM:, :].astype(F32), 0, keepdims=True) for r in refs]
    top = functools.reduce(jnp.maximum, logs)
    weights = [jnp.exp2(l - top) for l in logs]
    total = functools.reduce(jnp.add, weights)
    acc = jnp.zeros((HEAD_DIM, p0.shape[1]), F32)
    for r, w in zip(refs, weights):
        acc = acc + (w / total) * r[:HEAD_DIM, :].astype(F32)
    half = p0.shape[1] // 2
    is_first = lax.axis_index("space") % CORES == 0
    a, b = acc[:, :half], acc[:, half:]
    out[:HEAD_DIM, :] = jnp.where(is_first, a, b)
    out[HEAD_DIM:, :] = jnp.where(is_first, b, a)


def merge_heads(parts):
    return pl.pallas_call(
        merge_heads_kernel,
        in_specs=[VMEM] * 4,
        out_specs=VMEM,
        out_shape=shape((2 * HEAD_DIM, parts[0].shape[1] // 2), F32),
        compiler_params=PARAMS,
        cost_estimate=cost(1 << 20, 1 << 20),
        name="merge_heads",
    )(*parts)


def spread_kernel(both, _, out):
    value = both[...].T.astype(BF16)
    for i in range(out.shape[0]):
        out[i] = value


def spread(both, after, peers):
    return pl.pallas_call(
        spread_kernel,
        in_specs=[VMEM, ANY],
        out_specs=VMEM,
        out_shape=shape((peers, both.shape[1], both.shape[0]), BF16),
        compiler_params=PARAMS,
        cost_estimate=cost(1 << 20, 1 << 20),
        name="spread",
    )(both, after)


def trunk_kernel(mixed, w_mine, w_other, resid, gain, normed):
    heads = jnp.concatenate([mixed[i] for i in range(mixed.shape[0])], 1)
    weights = [ref[i] for i in range(mixed.shape[0]) for ref in (w_mine, w_other)]
    value = jnp.dot(heads, jnp.concatenate(weights, 0), preferred_element_type=F32)
    value = value + resid[...].astype(F32)
    mean = jnp.mean(value * value, -1, keepdims=True)
    normed[...] = (value * lax.rsqrt(mean + EPS) * gain[...]).astype(BF16)


def trunk(mixed, w_mine, w_other, resid, gain):
    return pl.pallas_call(
        trunk_kernel,
        in_specs=[VMEM] * 5,
        out_specs=VMEM,
        out_shape=shape(resid.shape, BF16),
        compiler_params=PARAMS,
        cost_estimate=cost(1 << 30, 4 << 20),
        name="trunk",
    )(mixed, w_mine, w_other, resid, gain)


def decode_kernel(normed, scale, shift, weight, out):
    each = out.shape[0]
    parts = []
    for i in range(each):
        v = pl.program_id(0) * each + i
        row = (1.0 + scale[pl.ds(v, 1), :], shift[pl.ds(v, 1), :])
        parts.append((normed[...].astype(F32) * row[0] + row[1]).astype(BF16))
    modulated = jnp.concatenate(parts, 0)
    result = jnp.dot(modulated, weight[...], preferred_element_type=F32).astype(BF16)
    out[...] = result.reshape(out.shape)


def decode(normed, scale, shift, weight):
    count, rows = scale.shape[0], normed.shape[0]
    each = 2
    return pl.pallas_call(
        decode_kernel,
        grid=(count // each,),
        in_specs=[VMEM] * 4,
        out_specs=pl.BlockSpec((each, rows, D), lambda v: (v, 0, 0)),
        out_shape=shape((count, rows, D), BF16),
        compiler_params=PARAMS,
        cost_estimate=cost(5 << 30, 8 << 20),
        name="decode",
    )(normed, scale, shift, weight)


def space_index(z, x, core):
    return (z * X + x) * CORES + core


def moves(step):
    return [
        (space_index(z, x, c), space_index(*step(z, x, c)))
        for z in range(Z_HI)
        for x in range(X)
        for c in range(CORES)
    ]


SWAP = moves(lambda z, x, c: (z, x, 1 - c))


def along_x(k):
    return moves(lambda z, x, c: (z, (x + k) % X, c))


def along_z(k):
    return moves(lambda z, x, c: ((z + k) % Z_HI, x, c))


def exchange(array):
    return lax.all_to_all(array, "chan", 0, 0, tiled=True)


def body(
    patches,
    var_embed,
    agg_query,
    pos_embed,
    gain_first,
    gain_second,
    w_qkv,
    w_out,
    w_dec,
    mod_scale,
    mod_shift,
):
    rows = patches.shape[1]
    peers = lax.axis_size("chan")

    parts = exchange(pool(patches, var_embed, agg_query.reshape(1, D), peers))
    resid = exchange(merge_pool(parts, pos_embed)).reshape(rows, D)

    kv, qt, copies = project(
        resid, gain_first.reshape(1, D), w_qkv.transpose(1, 0, 2), w_out, peers
    )
    key_pieces = [lax.ppermute(kv, "space", along_z(k)) for k in (2, 1, 3)]
    query_pieces = [lax.ppermute(qt, "space", along_x(k)) for k in (2, 1, 3)]
    w_mine = exchange(copies)
    key_pieces = [kv] + key_pieces
    key_pieces = key_pieces + [lax.ppermute(k, "space", SWAP) for k in key_pieces]
    back = []
    for k, piece in zip((2, 1, 3), query_pieces):
        partial = attend(key_pieces, piece)
        back.append(lax.ppermute(partial, "space", along_x(-k)))
    back.append(attend(key_pieces, qt))
    both = merge_heads(back)
    mixed = exchange(spread(both, w_mine, peers))
    w_other = lax.ppermute(w_mine, "space", SWAP)
    normed = trunk(mixed, w_mine, w_other, resid, gain_second.reshape(1, D))
    return decode(normed, mod_scale, mod_shift, w_dec)


def solution(mesh):
    placed = (
        P("chan", "space", None),
        P("chan", None),
        P(),
        P("space", None),
        P(),
        P(),
        P(None, None, "chan"),
        P("chan", None),
        P(),
        P("chan", None),
        P("chan", None),
    )

    return jax.shard_map(
        body, mesh=mesh, in_specs=placed, out_specs=P("chan", "space", None), check_vma=False
    )
```
